16 devices in a mesh: fsdp: 16 (over z, y, x, core).
Axes of the slice: x: 2, y: 2, z: 2, core: 2. Of those that a mesh axis runs over, the one named last changes fastest.
Arguments:
- tok_ids: int32 [16, 1536], P('fsdp')
- grad_out: bfloat16 [16, 1536, 1536], P('fsdp')
- emb_table: bfloat16 [151936, 1536], P('fsdp')
- norm_gain: bfloat16 [1536], P('fsdp')
- w_query: bfloat16 [1536, 1536], P('fsdp')
- b_query: bfloat16 [1536], P('fsdp')
- w_key: bfloat16 [1536, 256], P('fsdp')
- b_key: bfloat16 [256], P('fsdp')
- w_value: bfloat16 [1536, 256], P('fsdp')
- b_value: bfloat16 [256], P('fsdp')
- w_out: bfloat16 [1536, 1536], P('fsdp')
Outputs:
- output 1: bfloat16 [16, 1536, 1536], P('fsdp')
- output 2: bfloat16 [151936, 1536], P('fsdp')
- output 3: float32 [1536], P('fsdp')
- output 4: float32 [1536, 1536], P('fsdp')
- output 5: float32 [1536], P('fsdp')
- output 6: float32 [1536, 256], P('fsdp')
- output 7: float32 [256], P('fsdp')
- output 8: float32 [1536, 256], P('fsdp')
- output 9: float32 [256], P('fsdp')
- output 10: float32 [1536, 1536], P('fsdp')
All inputs are finite; a program needn't handle non-finite values.
Results may differ from the reference program's by a relative error of at most 0.0146869.
Values are sent between devices in bfloat16 or wider.
A program may use at most 1 GiB of HBM per device.

```python
import jax
import jax.numpy as jnp
from jax import lax

VOCAB = 151936
D_MODEL = 1536
HEADS = 12
KV_HEADS = 2
HEAD_DIM = 128
BATCH = 16
SEQ = 1536
HOT_IDS = 4096
ROPE_THETA = 1.0e6
NORM_EPS = 1e-6
MASK_VALUE = -1e30


def draw_ids(key_ids):
    key_pick, key_hot, key_wide = jax.random.split(key_ids, 3)
    pick_hot = jax.random.randint(key_pick, (BATCH, SEQ), 0, 2)
    low_ids = jax.random.randint(key_hot, (BATCH, SEQ), 0, HOT_IDS)
    hot_ids = (low_ids * low_ids) // HOT_IDS
    wide_ids = jax.random.randint(key_wide, (BATCH, SEQ), 0, VOCAB)
    tok_ids = jnp.where(pick_hot == 0, hot_ids, wide_ids).astype(jnp.int32)
    return tok_ids.at[0, SEQ - 1].set(VOCAB - 1)


def setup_inputs(seed: int = 0) -> dict:
    key_list = jax.random.split(jax.random.key(seed), 12)
    q_width = HEADS * HEAD_DIM
    kv_width = KV_HEADS * HEAD_DIM
    in_scale = D_MODEL ** -0.5
    out_scale = q_width ** -0.5

    def normal(key_n, shape):
        return jax.random.normal(key_n, shape, jnp.float32)

    return {
        "tok_ids": draw_ids(key_list[0]),
        "grad_out": normal(key_list[1], (BATCH, SEQ, D_MODEL)).astype(jnp.bfloat16),
        "emb_table": normal(key_list[2], (VOCAB, D_MODEL)).astype(jnp.bfloat16),
        "norm_gain": (1.0 + 0.3 * normal(key_list[3], (D_MODEL,))).astype(jnp.bfloat16),
        "w_query": (in_scale * normal(key_list[4], (D_MODEL, q_width))).astype(jnp.bfloat16),
        "b_query": (0.5 * normal(key_list[5], (q_width,))).astype(jnp.bfloat16),
        "w_key": (in_scale * normal(key_list[6], (D_MODEL, kv_width))).astype(jnp.bfloat16),
        "b_key": (0.5 * normal(key_list[7], (kv_width,))).astype(jnp.bfloat16),
        "w_value": (in_scale * normal(key_list[8], (D_MODEL, kv_width))).astype(jnp.bfloat16),
        "b_value": (0.5 * normal(key_list[9], (kv_width,))).astype(jnp.bfloat16),
        "w_out": (out_scale * normal(key_list[10], (q_width, D_MODEL))).astype(jnp.bfloat16),
    }


def rope_tables():
    half_dim = HEAD_DIM // 2
    inv_freq = jnp.power(ROPE_THETA, -(jnp.arange(half_dim, dtype=jnp.float32) * 2.0 / HEAD_DIM))
    angles = jnp.arange(SEQ, dtype=jnp.float32)[:, None] * inv_freq[None, :]
    angles = jnp.concatenate([angles, angles], axis=-1)
    return jnp.cos(angles)[:, None, :], jnp.sin(angles)[:, None, :]


def rotate(vector, cos_t, sin_t):
    half_dim = HEAD_DIM // 2
    turned = jnp.concatenate([-vector[..., half_dim:], vector[..., :half_dim]], axis=-1)
    return vector * cos_t + turned * sin_t


def block_seq(x_seq, params):
    gain_vec, w_query, b_query, w_key, b_key, w_value, b_value, w_out = params
    cos_t, sin_t = rope_tables()
    q_group = HEADS // KV_HEADS
    inv_rms = lax.rsqrt(jnp.mean(x_seq * x_seq, axis=-1, keepdims=True) + NORM_EPS)
    hidden = (x_seq * inv_rms * gain_vec).astype(jnp.bfloat16).astype(jnp.float32)
    q_lin = jnp.dot(hidden, w_query, preferred_element_type=jnp.float32) + b_query
    k_lin = jnp.dot(hidden, w_key, preferred_element_type=jnp.float32) + b_key
    v_lin = jnp.dot(hidden, w_value, preferred_element_type=jnp.float32) + b_value
    q_rot = rotate(q_lin.reshape(SEQ, HEADS, HEAD_DIM), cos_t, sin_t)
    q_rot = q_rot.astype(jnp.bfloat16).astype(jnp.float32).reshape(SEQ, KV_HEADS, q_group, HEAD_DIM)
    k_rot = rotate(k_lin.reshape(SEQ, KV_HEADS, HEAD_DIM), cos_t, sin_t)
    k_rot = k_rot.astype(jnp.bfloat16).astype(jnp.float32)
    v_val = v_lin.reshape(SEQ, KV_HEADS, HEAD_DIM).astype(jnp.bfloat16).astype(jnp.float32)
    scores = jnp.einsum("qkgd,skd->kgqs", q_rot, k_rot) * (HEAD_DIM ** -0.5)
    causal = jnp.arange(SEQ)[:, None] >= jnp.arange(SEQ)[None, :]
    scores = jnp.where(causal, scores, MASK_VALUE)
    prob_b = jax.nn.softmax(scores, axis=-1).astype(jnp.bfloat16).astype(jnp.float32)
    attn_out = jnp.einsum("kgqs,skd->qkgd", prob_b, v_val).reshape(SEQ, HEADS * HEAD_DIM)
    attn_out = attn_out.astype(jnp.bfloat16).astype(jnp.float32)
    proj_out = jnp.dot(attn_out, w_out, preferred_element_type=jnp.float32)
    return (x_seq + proj_out).astype(jnp.bfloat16)


def reference(tok_ids, grad_out, emb_table, norm_gain, w_query, b_query, w_key, b_key, w_value, b_value, w_out):
    x_all = jnp.take(emb_table, tok_ids, axis=0).astype(jnp.float32)
    params = tuple(weight.astype(jnp.float32) for weight in (norm_gain, w_query, b_query, w_key, b_key, w_value, b_value, w_out))
    seq_step = jax.checkpoint(block_seq)

    def forward(x_in, prm_list):
        return lax.map(lambda x_seq: seq_step(x_seq, prm_list), x_in)

    block_out, pullback = jax.vjp(forward, x_all, params)
    d_x, d_params = pullback(grad_out)
    grad_table = jax.ops.segment_sum(d_x.reshape(-1, D_MODEL), tok_ids.reshape(-1), num_segments=VOCAB)
    grad_table = grad_table.astype(jnp.bfloat16)
    return (block_out, grad_table, d_params[0], d_params[1], d_params[2], d_params[3], d_params[4], d_params[5], d_params[6], d_params[7])
```

```python
import functools

import jax
import jax.numpy as jnp
from jax import lax
from jax.experimental import pallas as pl
from jax.experimental.pallas import tpu as pltpu
from jax.sharding import PartitionSpec as P

HEAD_DIM = 128
ROPE_THETA = 1.0e6
NORM_EPS = 1e-6
MASK_VALUE = -1e30
N_DEV = 16
HOT_IDS = 4096
HOT_ROWS = HOT_IDS // N_DEV
HOT_GROUPS = HOT_IDS // (N_DEV * 8)
CAP = 144
Q_BLOCK = 256
ROW_BLOCK = 256
F32 = jnp.float32
BF16 = jnp.bfloat16
MESH_ID = pl.DeviceIdType.MESH
VMEM_LIMIT = 60 * 1024 * 1024


def rope_tables(seq_len):
    half_dim = HEAD_DIM // 2
    inv_freq = jnp.power(ROPE_THETA, -(jnp.arange(half_dim, dtype=F32) * 2.0 / HEAD_DIM))
    angles = jnp.arange(seq_len, dtype=F32)[:, None] * inv_freq[None, :]
    cos_h, sin_h = jnp.cos(angles), jnp.sin(angles)
    return jnp.concatenate([cos_h, cos_h], axis=-1), jnp.concatenate([-sin_h, sin_h], axis=-1)


def all_barrier():
    me = lax.axis_index("fsdp")
    barrier = pltpu.get_barrier_semaphore()
    for k in range(1, N_DEV):
        pl.semaphore_signal(barrier, inc=1, device_id=(lax.rem(me + k, N_DEV),), device_id_type=MESH_ID)
    pl.semaphore_wait(barrier, N_DEV - 1)


def head_exchange_kernel(table_ref, req_ref, small_ref, hot_ref, reqs_ref, smalls_ref, bounce, send_q, recv_q, send_s, recv_s, send_h, recv_h, local):
    me = lax.axis_index("fsdp")
    all_barrier()
    copies = []
    for k in range(1, N_DEV):
        to = lax.rem(me + k, N_DEV)
        copies.append(pltpu.make_async_remote_copy(req_ref.at[to], reqs_ref.at[me], send_q.at[k], recv_q.at[k], (to,), MESH_ID))
        copies.append(pltpu.make_async_remote_copy(small_ref, smalls_ref.at[me], send_s.at[k], recv_s.at[k], (to,), MESH_ID))
    for copy in copies:
        copy.start()

    @pl.when(me == 0)
    def _():
        hot_copies = []
        for k in range(1, N_DEV):
            hot_copies.append(pltpu.make_async_remote_copy(table_ref.at[pl.ds(0, HOT_GROUPS), k], hot_ref, send_h.at[k], recv_h, (k,), MESH_ID))
        for copy in hot_copies:
            copy.start()
        mine = pltpu.make_async_copy(table_ref.at[pl.ds(0, HOT_GROUPS), 0], bounce, local)
        mine.start()
        mine.wait()
        mine = pltpu.make_async_copy(bounce, hot_ref, local)
        mine.start()
        mine.wait()
        for copy in hot_copies:
            copy.wait_send()

    reqs_ref[me] = req_ref[me]
    smalls_ref[me] = small_ref[...]

    @pl.when(me != 0)
    def _():
        pltpu.make_async_remote_copy(table_ref.at[pl.ds(0, HOT_GROUPS), 0], hot_ref, send_h.at[0], recv_h, (0,), MESH_ID).wait_recv()

    for copy in copies:
        copy.wait()


def head_exchange(table_part, requests, small_vec):
    rows_dev, width = table_part.shape
    table_view = table_part[:HOT_IDS].reshape(HOT_GROUPS, N_DEV, 8, width)
    any_spec = pl.BlockSpec(memory_space=pl.ANY)
    vmem_spec = pl.BlockSpec(memory_space=pltpu.VMEM)
    return pl.pallas_call(
        head_exchange_kernel,
        out_shape=(
            jax.ShapeDtypeStruct((HOT_GROUPS, 8, width), BF16),
            jax.ShapeDtypeStruct((N_DEV,) + requests.shape[1:], jnp.int32),
            jax.ShapeDtypeStruct((N_DEV,) + small_vec.shape, F32),
        ),
        in_specs=[any_spec, vmem_spec, vmem_spec],
        out_specs=(any_spec, vmem_spec, vmem_spec),
        scratch_shapes=[pltpu.VMEM((HOT_GROUPS, 8, width), BF16)]
        + [pltpu.SemaphoreType.DMA((N_DEV,))] * 5
        + [pltpu.SemaphoreType.DMA, pltpu.SemaphoreType.DMA],
        compiler_params=pltpu.CompilerParams(collective_id=1, has_side_effects=True),
        name="head_exchange",
    )(table_view, requests, small_vec)


def hot_return_kernel(sums_ref, out_ref, send_h, recv_h, local, bounce):
    me = lax.axis_index("fsdp")
    all_barrier()

    @pl.when(me == 0)
    def _():
        mine = pltpu.make_async_copy(sums_ref, bounce, local)
        mine.start()
        mine.wait()
        mine = pltpu.make_async_copy(bounce, out_ref.at[:, 0], local)
        mine.start()
        mine.wait()
        for k in range(1, N_DEV):
            pltpu.make_async_remote_copy(sums_ref, out_ref.at[:, k], send_h, recv_h.at[k], (k,), MESH_ID).wait_recv()

    @pl.when(me != 0)
    def _():
        copy = pltpu.make_async_remote_copy(sums_ref, out_ref.at[:, me], send_h, recv_h.at[me], (0,), MESH_ID)
        copy.start()
        copy.wait_send()


def hot_return(hot_sums):
    groups, _, width = hot_sums.shape
    any_spec = pl.BlockSpec(memory_space=pl.ANY)
    return pl.pallas_call(
        hot_return_kernel,
        out_shape=jax.ShapeDtypeStruct((groups, N_DEV, 8, width), BF16),
        in_specs=[any_spec],
        out_specs=any_spec,
        scratch_shapes=[
            pltpu.SemaphoreType.DMA,
            pltpu.SemaphoreType.DMA((N_DEV,)),
            pltpu.SemaphoreType.DMA,
            pltpu.VMEM((groups, 8, width), BF16),
        ],
        compiler_params=pltpu.CompilerParams(collective_id=2, has_side_effects=True),
        name="hot_return",
    )(hot_sums)


def qkv_kernel(x_ref, w_ref, gain_ref, bias_ref, cos_ref, sin_ref, hidden_ref, qkv_ref):
    x_f = x_ref[...].astype(F32)
    inv_rms = lax.rsqrt(jnp.mean(x_f * x_f, axis=-1, keepdims=True) + NORM_EPS)
    hidden = (x_f * inv_rms * gain_ref[...]).astype(BF16)
    hidden_ref[...] = hidden
    cos_t, sin_t = cos_ref[...], sin_ref[...]
    n_rot = qkv_ref.shape[1] // HEAD_DIM
    for c in range(n_rot // 2):
        cols = pl.ds(c * 2 * HEAD_DIM, 2 * HEAD_DIM)
        lin = jnp.dot(hidden, w_ref[:, cols], preferred_element_type=F32) + bias_ref[:, cols]
        for j in range(2):
            head = 2 * c + j
            vec = lin[:, j * HEAD_DIM : (j + 1) * HEAD_DIM]
            if head < 12 or head in (12, 14):
                vec = vec * cos_t + pltpu.roll(vec, HEAD_DIM // 2, 1) * sin_t
            qkv_ref[:, head * HEAD_DIM : (head + 1) * HEAD_DIM] = vec.astype(BF16)


def qkv_proj(x_rows, w_all, gain_row, bias_row, cos_t, sin_t):
    seq_len, width = x_rows.shape
    cols = bias_row.shape[1]
    return pl.pallas_call(
        qkv_kernel,
        grid=(seq_len // ROW_BLOCK,),
        out_shape=(jax.ShapeDtypeStruct((seq_len, width), BF16), jax.ShapeDtypeStruct((seq_len, cols), BF16)),
        in_specs=[
            pl.BlockSpec((ROW_BLOCK, width), lambda i: (i, 0)),
            pl.BlockSpec((width, cols), lambda i: (0, 0)),
            pl.BlockSpec((1, width), lambda i: (0, 0)),
            pl.BlockSpec((1, cols), lambda i: (0, 0)),
            pl.BlockSpec((ROW_BLOCK, HEAD_DIM), lambda i: (i, 0)),
            pl.BlockSpec((ROW_BLOCK, HEAD_DIM), lambda i: (i, 0)),
        ],
        out_specs=(pl.BlockSpec((ROW_BLOCK, width), lambda i: (i, 0)), pl.BlockSpec((ROW_BLOCK, cols), lambda i: (i, 0))),
        compiler_params=pltpu.CompilerParams(vmem_limit_bytes=VMEM_LIMIT),
        cost_estimate=pl.CostEstimate(flops=2 * seq_len * width * cols, bytes_accessed=20_000_000, transcendentals=0),
        name="qkv_proj",
    )(x_rows, w_all, gain_row, bias_row, cos_t, sin_t)


def attention_kernel(q_ref, k_ref, v_ref, do_ref, cosq_ref, sinq_ref, cosk_ref, sink_ref, o_ref, dq_ref, dkv_ref, dbq_ref, dbkv_ref, dk_acc, dv_acc, kt_ref, vt_ref):
    h_step, q_step = pl.program_id(1), pl.program_id(2)
    n_q = pl.num_programs(2)
    scale = HEAD_DIM**-0.5

    @pl.when((h_step == 0) & (q_step == 0))
    def _():
        dk_acc[...] = jnp.zeros_like(dk_acc)
        dv_acc[...] = jnp.zeros_like(dv_acc)
        kt_ref[...] = k_ref[...].T
        vt_ref[...] = v_ref[...].T

    q_blk, do_blk = q_ref[...], do_ref[...]
    last_dims = (((1,), (1,)), ((), ()))

    def step(length):
        s_t = lax.dot_general(k_ref[:length, :], q_blk, last_dims, preferred_element_type=F32) * scale
        key_pos = lax.broadcasted_iota(jnp.int32, (Q_BLOCK, Q_BLOCK), 0)
        query_pos = lax.broadcasted_iota(jnp.int32, (Q_BLOCK, Q_BLOCK), 1)
        diag = jnp.where(query_pos >= key_pos, s_t[length - Q_BLOCK :], MASK_VALUE)
        s_t = diag if length == Q_BLOCK else jnp.concatenate([s_t[: length - Q_BLOCK], diag], axis=0)
        top = jnp.max(s_t, axis=0, keepdims=True)
        e_t = jnp.exp(s_t - top)
        p_t = e_t * (1.0 / jnp.sum(e_t, axis=0, keepdims=True))
        p_b = p_t.astype(BF16)
        o_ref[...] = jnp.dot(vt_ref[:, :length], p_b, preferred_element_type=F32).T.astype(BF16)
        dp_t = lax.dot_general(v_ref[:length, :], do_blk, last_dims, preferred_element_type=F32)
        delta = jnp.sum(dp_t * p_t, axis=0, keepdims=True)
        ds_b = (p_t * (dp_t - delta) * scale).astype(BF16)
        dv_acc[:length, :] += jnp.dot(p_b, do_blk, preferred_element_type=F32)
        dk_acc[:length, :] += jnp.dot(ds_b, q_blk, preferred_element_type=F32)
        dq = jnp.dot(kt_ref[:, :length], ds_b, preferred_element_type=F32).T
        dq = dq * cosq_ref[...] - pltpu.roll(dq, HEAD_DIM // 2, 1) * sinq_ref[...]
        dq_ref[...] = dq.astype(BF16)
        part = jnp.sum(dq, axis=0, keepdims=True)
        dbq_ref[0] = part if length == Q_BLOCK else dbq_ref[0] + part

    for i in range(k_ref.shape[0] // Q_BLOCK):
        pl.when(q_step == i)(functools.partial(step, (i + 1) * Q_BLOCK))

    @pl.when((h_step == pl.num_programs(1) - 1) & (q_step == n_q - 1))
    def _():
        dk = dk_acc[...]
        dk = dk * cosk_ref[...] - pltpu.roll(dk, HEAD_DIM // 2, 1) * sink_ref[...]
        dv = dv_acc[...]
        dkv_ref[:, :HEAD_DIM] = dk.astype(BF16)
        dkv_ref[:, HEAD_DIM:] = dv.astype(BF16)
        dbkv_ref[0, :, :HEAD_DIM] = jnp.sum(dk, axis=0, keepdims=True)
        dbkv_ref[0, :, HEAD_DIM:] = jnp.sum(dv, axis=0, keepdims=True)


def attention(qkv, d_attn, cos_t, sin_t, n_heads, kv_heads):
    seq_len = qkv.shape[0]
    group = n_heads // kv_heads
    grid = (kv_heads, group, seq_len // Q_BLOCK)
    head_blk = pl.BlockSpec((Q_BLOCK, HEAD_DIM), lambda g, h, i: (i, g * group + h))
    rope_q = pl.BlockSpec((Q_BLOCK, HEAD_DIM), lambda g, h, i: (i, 0))
    rope_k = pl.BlockSpec((seq_len, HEAD_DIM), lambda g, h, i: (0, 0))
    return pl.pallas_call(
        attention_kernel,
        grid=grid,
        out_shape=(
            jax.ShapeDtypeStruct((seq_len, n_heads * HEAD_DIM), BF16),
            jax.ShapeDtypeStruct((seq_len, n_heads * HEAD_DIM), BF16),
            jax.ShapeDtypeStruct((seq_len, 2 * kv_heads * HEAD_DIM), BF16),
            jax.ShapeDtypeStruct((n_heads, 1, HEAD_DIM), F32),
            jax.ShapeDtypeStruct((kv_heads, 1, 2 * HEAD_DIM), F32),
        ),
        in_specs=[
            head_blk,
            pl.BlockSpec((seq_len, HEAD_DIM), lambda g, h, i: (0, n_heads + 2 * g)),
            pl.BlockSpec((seq_len, HEAD_DIM), lambda g, h, i: (0, n_heads + 2 * g + 1)),
            head_blk,
            rope_q,
            rope_q,
            rope_k,
            rope_k,
        ],
        out_specs=(
            head_blk,
            head_blk,
            pl.BlockSpec((seq_len, 2 * HEAD_DIM), lambda g, h, i: (0, g)),
            pl.BlockSpec((1, 1, HEAD_DIM), lambda g, h, i: (g * group + h, 0, 0)),
            pl.BlockSpec((1, 1, 2 * HEAD_DIM), lambda g, h, i: (g, 0, 0)),
        ),
        scratch_shapes=[
            pltpu.VMEM((seq_len, HEAD_DIM), F32),
            pltpu.VMEM((seq_len, HEAD_DIM), F32),
            pltpu.VMEM((HEAD_DIM, seq_len), BF16),
            pltpu.VMEM((HEAD_DIM, seq_len), BF16),
        ],
        compiler_params=pltpu.CompilerParams(vmem_limit_bytes=VMEM_LIMIT),
        cost_estimate=pl.CostEstimate(flops=6 * 2 * n_heads * seq_len * seq_len * HEAD_DIM, bytes_accessed=25_000_000, transcendentals=0),
        name="attention",
    )(qkv, qkv, qkv, d_attn, cos_t, sin_t, cos_t, sin_t)


def dx_kernel(dq_ref, dkv_ref, w_ref, x_ref, go_ref, gain_ref, dx_ref, dqkv_ref, dgain_ref):
    q_cols = dq_ref.shape[1]
    last_dims = (((1,), (1,)), ((), ()))
    dq, dkv = dq_ref[...], dkv_ref[...]
    dqkv_ref[:, :q_cols] = dq
    dqkv_ref[:, q_cols:] = dkv
    d_hidden = lax.dot_general(dq, w_ref[:, :q_cols], last_dims, preferred_element_type=F32)
    d_hidden += lax.dot_general(dkv, w_ref[:, q_cols:], last_dims, preferred_element_type=F32)
    x_f = x_ref[...].astype(F32)
    inv_rms = lax.rsqrt(jnp.mean(x_f * x_f, axis=-1, keepdims=True) + NORM_EPS)
    x_norm = x_f * inv_rms
    part = jnp.sum(d_hidden * x_norm, axis=0, keepdims=True)
    first = pl.program_id(0) == 0
    dgain_ref[...] = jnp.where(first, part, dgain_ref[...] + part)
    d_norm = d_hidden * gain_ref[...]
    d_x = inv_rms * (d_norm - x_norm * jnp.mean(d_norm * x_norm, axis=-1, keepdims=True))
    dx_ref[...] = go_ref[...].astype(F32) + d_x


def input_grad(dq_b, dkv_b, w_all, x_rows, grad_out, gain_row):
    seq_len, width = x_rows.shape
    q_cols, kv_cols = dq_b.shape[1], dkv_b.shape[1]
    cols = q_cols + kv_cols
    row_blk = pl.BlockSpec((ROW_BLOCK, width), lambda i: (i, 0))
    return pl.pallas_call(
        dx_kernel,
        grid=(seq_len // ROW_BLOCK,),
        out_shape=(
            jax.ShapeDtypeStruct((seq_len, width), F32),
            jax.ShapeDtypeStruct((seq_len, cols), BF16),
            jax.ShapeDtypeStruct((1, width), F32),
        ),
        in_specs=[
            pl.BlockSpec((ROW_BLOCK, q_cols), lambda i: (i, 0)),
            pl.BlockSpec((ROW_BLOCK, kv_cols), lambda i: (i, 0)),
            pl.BlockSpec((width, cols), lambda i: (0, 0)),
            row_blk,
            row_blk,
            pl.BlockSpec((1, width), lambda i: (0, 0)),
        ],
        out_specs=(row_blk, pl.BlockSpec((ROW_BLOCK, cols), lambda i: (i, 0)), pl.BlockSpec((1, width), lambda i: (0, 0))),
        compiler_params=pltpu.CompilerParams(vmem_limit_bytes=VMEM_LIMIT),
        cost_estimate=pl.CostEstimate(flops=2 * seq_len * width * cols, bytes_accessed=40_000_000, transcendentals=0),
        name="input_grad",
    )(dq_b, dkv_b, w_all, x_rows, grad_out, gain_row)


def routing(ids, rows_dev):
    agg = jnp.where(ids < HOT_IDS, (ids // 8) % N_DEV, ids // rows_dev)
    pos = jnp.arange(ids.shape[0], dtype=jnp.int32)
    same = ids[:, None] == ids[None, :]
    first = ~jnp.any(same & (pos[:, None] < pos[None, :]), axis=0)
    lower = first[:, None] & (agg[:, None] == agg[None, :]) & (ids[:, None] < ids[None, :])
    slot = jnp.sum(lower.astype(jnp.int32), axis=0)
    place = jnp.where(first & (slot < CAP), agg * CAP + slot, N_DEV * CAP)
    slots = jnp.arange(N_DEV * CAP, dtype=jnp.int32)
    requests = jnp.sum(jnp.where(place[:, None] == slots[None, :], ids[:, None] + 1, 0), axis=0)
    return agg, slot, requests.reshape(N_DEV, 1, CAP), jnp.max(slot) + 1


def solution(mesh):
    row_spec = P("fsdp", None)
    vec_spec = P("fsdp")
    act_spec = P("fsdp", None, None)
    weight_specs = (vec_spec, row_spec, vec_spec, row_spec, vec_spec, row_spec, vec_spec, row_spec)
    in_specs = (row_spec, act_spec, row_spec) + weight_specs
    out_specs = (act_spec, row_spec) + weight_specs

    def device_step(tok_ids, grad_out, table_part, gain_part, wq_part, bq_part, wk_part, bk_part, wv_part, bv_part, wo_part):
        rows_dev, width = table_part.shape
        q_cols, kv_cols = wq_part.shape[1], wk_part.shape[1]
        n_heads, kv_heads = q_cols // HEAD_DIM, kv_cols // HEAD_DIM
        seq_len = tok_ids.shape[1]
        me = lax.axis_index("fsdp")
        first_row = me * rows_dev
        ids = tok_ids[0]
        grad_seq = grad_out[0]

        def kv_order(k_arr, v_arr):
            parts = []
            for g in range(kv_heads):
                parts += [k_arr[..., g * HEAD_DIM : (g + 1) * HEAD_DIM], v_arr[..., g * HEAD_DIM : (g + 1) * HEAD_DIM]]
            return parts

        wqkv_full = lax.all_gather(jnp.concatenate([wq_part] + kv_order(wk_part, wv_part), axis=1), "fsdp", axis=0, tiled=True)
        wo_full = lax.all_gather(wo_part, "fsdp", axis=0, tiled=True)
        cos_t, sin_t = rope_tables(seq_len)

        agg, slot, requests, most = routing(ids, rows_dev)
        small = jnp.concatenate([gain_part, bq_part, bk_part, bv_part]).astype(F32)
        n_small = small.shape[0]
        small = jnp.concatenate([small, most.astype(F32)[None], jnp.zeros((256 - n_small - 1,), F32)])[None]
        hot_rows, wanted, smalls = head_exchange(table_part, requests, small)
        smalls = smalls[:, 0]
        n_g, n_q, n_kv = gain_part.shape[0], bq_part.shape[0], bk_part.shape[0]
        gain_row = smalls[:, :n_g].reshape(1, width)
        bq_full = smalls[:, n_g : n_g + n_q].reshape(q_cols)
        bk_full = smalls[:, n_g + n_q : n_g + n_q + n_kv].reshape(kv_cols)
        bv_full = smalls[:, n_g + n_q + n_kv : n_small].reshape(kv_cols)
        bias_row = jnp.concatenate([bq_full] + kv_order(bk_full, bv_full))[None]
        fits = jnp.max(smalls[:, n_small]) <= CAP

        wanted = wanted.reshape(N_DEV * CAP) - 1
        asked = wanted >= 0
        is_hot = wanted < HOT_IDS
        hot_idx = jnp.where(asked & is_hot, (wanted // (8 * N_DEV)) * 8 + wanted % 8, 0)
        cold_idx = jnp.where(asked & ~is_hot, wanted - first_row, 0)
        token_place = agg * CAP + jnp.minimum(slot, CAP - 1)

        def owned_index():
            all_ids = lax.all_gather(ids, "fsdp")
            local_idx = all_ids - first_row
            return local_idx, (local_idx >= 0) & (local_idx < rows_dev)

        def lookup_fast():
            cold = jnp.take(table_part, cold_idx, axis=0)
            hot = jnp.take(hot_rows.reshape(HOT_ROWS, width), hot_idx, axis=0)
            send = jnp.where((asked & is_hot)[:, None], hot, cold).reshape(N_DEV, CAP, width)
            got = lax.all_to_all(send, "fsdp", 0, 0, tiled=True)
            return jnp.take(got.reshape(N_DEV * CAP, width), token_place, axis=0)

        def lookup_dense():
            local_idx, is_owned = owned_index()
            looked = jnp.take(table_part, jnp.where(is_owned, local_idx, 0), axis=0)
            looked = jnp.where(is_owned[..., None], looked, jnp.zeros((), BF16))
            return lax.psum_scatter(looked, "fsdp", scatter_dimension=0)

        x_rows = lax.cond(fits, lookup_fast, lookup_dense)

        d_attn = lax.dot_general(grad_seq, wo_full, (((1,), (1,)), ((), ())), preferred_element_type=F32).astype(BF16)
        hidden, qkv = qkv_proj(x_rows, wqkv_full, gain_row, bias_row, cos_t, sin_t)
        attn_b, dq_b, dkv_b, dbq, dbkv = attention(qkv, d_attn, cos_t, sin_t, n_heads, kv_heads)
        d_x, dqkv_b, dgain = input_grad(dq_b, dkv_b, wqkv_full, x_rows, grad_seq, gain_row)

        rows_dims = (((0,), (0,)), ((), ()))
        grad_wo = lax.dot_general(attn_b, grad_seq, rows_dims, preferred_element_type=F32)
        grad_wqkv = lax.dot_general(hidden, dqkv_b, rows_dims, preferred_element_type=F32)
        proj_out = jnp.dot(attn_b, wo_full, preferred_element_type=F32)
        block_out = (x_rows.astype(F32) + proj_out).astype(BF16)
        grad_wo = lax.psum_scatter(grad_wo, "fsdp", scatter_dimension=0, tiled=True)
        grad_wqkv = lax.psum_scatter(grad_wqkv, "fsdp", scatter_dimension=0, tiled=True)

        def table_fast():
            packed = jnp.zeros((N_DEV * CAP, width), F32).at[token_place].add(d_x)
            got = lax.all_to_all(packed.reshape(N_DEV, CAP, width), "fsdp", 0, 0, tiled=True).reshape(N_DEV * CAP, width)
            dest = jnp.where(asked, jnp.where(is_hot, rows_dev + hot_idx, cold_idx), rows_dev + HOT_ROWS)
            summed = jnp.zeros((rows_dev + HOT_ROWS, width), F32).at[dest].add(got, mode="drop")
            hot_sums = summed[rows_dev:].astype(BF16).reshape(HOT_GROUPS, 8, width)
            returned = hot_return(hot_sums).reshape(HOT_IDS, width)
            low = jnp.where(me == 0, returned, summed[:HOT_IDS].astype(BF16))
            return jnp.concatenate([low, summed[HOT_IDS:rows_dev].astype(BF16)], axis=0)

        def table_dense():
            local_idx, is_owned = owned_index()
            all_dx = lax.all_gather(d_x, "fsdp")
            seg_idx = jnp.where(is_owned, local_idx, rows_dev)
            return jax.ops.segment_sum(all_dx.reshape(-1, width), seg_idx.reshape(-1), num_segments=rows_dev).astype(BF16)

        grad_table = lax.cond(fits, table_fast, table_dense)

        def kv_split(arr):
            ks = [arr[..., 2 * g * HEAD_DIM : (2 * g + 1) * HEAD_DIM] for g in range(kv_heads)]
            vs = [arr[..., (2 * g + 1) * HEAD_DIM : (2 * g + 2) * HEAD_DIM] for g in range(kv_heads)]
            return jnp.concatenate(ks, axis=-1), jnp.concatenate(vs, axis=-1)

        dbk, dbv = kv_split(dbkv.reshape(2 * kv_cols))
        vecs = jnp.concatenate(
            [dgain.reshape(N_DEV, n_g), dbq.reshape(N_DEV, n_q), dbk.reshape(N_DEV, n_kv), dbv.reshape(N_DEV, n_kv)], axis=1
        )
        vecs = lax.psum_scatter(vecs, "fsdp", scatter_dimension=0, tiled=True)[0]
        grad_wk, grad_wv = kv_split(grad_wqkv[:, q_cols:])
        return (
            block_out[None],
            grad_table,
            vecs[:n_g],
            grad_wqkv[:, :q_cols],
            vecs[n_g : n_g + n_q],
            grad_wk,
            vecs[n_g + n_q : n_g + n_q + n_kv],
            grad_wv,
            vecs[n_g + n_q + n_kv : n_small],
            grad_wo,
        )

    return jax.shard_map(device_step, mesh=mesh, in_specs=in_specs, out_specs=out_specs, check_vma=False)
```
